32 devices in a mesh: shuf: 8 (over z, y), rep: 4 (over x, core).
Axes of the slice: x: 2, y: 2, z: 4, core: 2. Of those that a mesh axis runs over, the one named last changes fastest.
Arguments:
- values: bfloat16 [65536, 1024], P('shuf', 'rep')
- subgroup: int32 [512], P('shuf'), may hold values from 0 to 31
- owners: int32 [512, 1], P('shuf'), may hold values from 0 to 7; in each aligned block of 64 rows (0 to 63, 64 to 127, ...) at most 16 rows name the same one
- col_gain: float32 [1024], P('rep'), may hold values from 0.5 to 1.5
- col_bias: float32 [1024], P('rep'), may hold values from -3 to 3
- out_weight: bfloat16 [1024, 1024], P('rep'), may hold values from -0.1875 to 0.1875
Outputs:
- projected: bfloat16 [65536, 1024], P(('shuf', 'rep'))
The draws below stay inside these ranges and needn't reach their ends.
Inputs may be any that keep to these rules, and one draw needn't show every extreme that they name: `owners`: among the tiles of one index of shuf no owner is named more than 16 times, a bound that some block reaches.
All inputs are finite; a program needn't handle non-finite values.
Results may differ from the reference program's by a relative error of at most 0.015.
Values may be sent and summed in bfloat16 or wider, within the bound.
A program may use at most 64 MiB of HBM per device.

```python
import math
import jax
import jax.numpy as jnp
import numpy as np
from jax import lax

TILE = 128
TILES_DEV = 64
COLS = 1024
OUT = 1024
GRP_DEV = 32
PRIOR = 256
ROWS_DEV = 8192
TILES = 512
ROWS = 65536
CAP = 16
N_SHUF = 8
N_REP = 4


def draw_values(key, part):
    keys = jax.random.split(jax.random.fold_in(key, 11), 7)
    blocks = ROWS // ROWS_DEV
    place = jnp.arange(ROWS, dtype=jnp.float32).reshape(TILES, TILE, 1) / float(ROWS)
    rough = jax.random.uniform(keys[0], (TILES, TILE, 1), minval=0.7, maxval=1.4)
    row_scale = jnp.exp(jnp.log(3.0) * place) * rough
    shift = 1.5 * jax.random.normal(keys[4], (blocks, 1, COLS))
    shift_rows = jnp.repeat(shift, TILES_DEV, axis=0)
    chosen = jax.random.bernoulli(keys[5], 0.5, (TILES, 1, COLS))
    stretch = jnp.exp(jax.random.uniform(keys[6], (TILES, 1, COLS), minval=-0.6, maxval=0.6))
    factor = jnp.where(chosen, stretch, 1.0)
    col_scale = jnp.exp(jax.random.uniform(keys[1], (1, 1, COLS), minval=0.0, maxval=jnp.log(10.0)))
    noise = jax.random.normal(keys[2], (TILES, TILE, COLS))
    offset = jax.random.normal(keys[3], (1, 1, COLS)) * (0.5 + 2.0 * place)
    drawn = col_scale * (offset + shift_rows + row_scale * noise * factor)
    return drawn.reshape(ROWS, COLS).astype(jnp.bfloat16)


def set_ends(values, stream_key, low, largest):
    spot = [jax.random.randint(jax.random.fold_in(stream_key, axis), (), 0, length) for axis, length in enumerate(values.shape)]
    widest = values.shape.index(max(values.shape))
    beside = spot[:widest] + [(spot[widest] + 1) % values.shape[widest]] + spot[widest + 1:]
    return values.at[tuple(spot)].set(low).at[tuple(beside)].set(largest)


def level_of(own_key, dims, pieces, smallest, high):
    gain, own = 1.0, jax.random.fold_in(own_key, 6)
    for axis_at, parts in pieces:
        heights = jnp.exp(jax.random.uniform(jax.random.fold_in(own, axis_at), (parts,), jnp.float32, smallest / len(pieces), high / len(pieces)))
        gain = gain * jnp.repeat(heights, dims[axis_at] // parts).reshape([-1 if axis == axis_at else 1 for axis in range(len(dims))])
    return gain


def assign_block(key, own, number, rows, amount, top, most, slope):
    sequence = jax.random.permutation(key, amount)
    heavy_load, ordinary = load_shares(amount, rows * top, most, slope, True), load_shares(amount, rows * top, most, slope, False)
    places = jnp.arange(amount)

    def named(tallies, offset_by):
        used = int((tallies > 0).sum())
        fixed = max(1, used // 4)
        passed = fixed + (places - fixed + offset_by * (used - fixed)) % max(1, amount - fixed)
        return jnp.zeros((amount,), jnp.int32).at[sequence[jnp.where(places < fixed, places, passed)]].set(jnp.asarray(tallies, jnp.int32))

    tallies = jnp.where(number % 4 == 0, named(heavy_load, number // 4), named(ordinary, number - number // 4 - 1))
    mixed = jax.random.permutation(jax.random.fold_in(own, 3), amount)
    source_of, sink = mixed[0:amount // 2 * 2:2], mixed[1:amount // 2 * 2:2]
    margin = jnp.minimum(tallies[source_of] - 1, most - tallies[sink]) // 2
    margin = jnp.where((source_of == sequence[0]) | (sink == sequence[0]) | (tallies[sink] == 0), 0, jnp.maximum(margin, 0))
    passed = jax.random.randint(jax.random.fold_in(own, 4), (amount // 2,), 0, 1 << 20) % (margin + 1)
    tallies = tallies.at[source_of].add(-passed).at[sink].add(passed)
    labels = jnp.searchsorted(jnp.cumsum(tallies), jnp.arange(rows * top), side="right").astype(jnp.int32)
    listing = labels.reshape(top, rows).T
    listing = listing[jax.random.permutation(jax.random.fold_in(own, 1), rows)]
    offset_by = jax.random.randint(jax.random.fold_in(own, 2), (rows, 1), 0, top)
    return jnp.take_along_axis(listing, (jnp.arange(top)[None, :] + offset_by) % top, axis=1)


def load_shares(count, total, limit, slope, full):
    portions = [(1 << 20) // math.isqrt(rank ** slope) + 1 for rank in range(1, count + 1)]
    largest = limit if full else min(limit, max(-(-total // count), total * portions[0] // sum(portions)))
    least = 1 if total - largest >= count - 1 else 0
    counts, surplus = [largest] + [least] * (count - 1), total - largest - least * (count - 1)
    while surplus > 0:
        movable = [i for i in range(1, count) if counts[i] < largest] or [i for i in range(1, count) if counts[i] < limit]
        whole, remaining = sum([portions[i] for i in movable]), surplus
        for i in movable:
            more = min(limit - counts[i], max(1, remaining * portions[i] // whole), surplus)
            counts[i] = counts[i] + more
            surplus = surplus - more
    return np.array(counts)


def normal_values(stream_key, extent, scale, reach, shards=(), held_as=jnp.bfloat16):
    result = scale * jax.random.normal(stream_key, extent, jnp.float32)
    if shards:
        result = result * level_of(stream_key, extent, shards, -0.22, 0.18)
    return jnp.clip(result, -reach, reach).astype(held_as)


def setup_inputs(seed: int = 0) -> dict:
    key_list = jax.random.split(jax.random.key(seed), 7)
    values = draw_values(jax.random.fold_in(key_list[6], 71), 0)
    subgroup = set_ends(jax.random.randint(key_list[1], (TILES,), 0, GRP_DEV), jax.random.fold_in(key_list[1], 1), 0, GRP_DEV - 1).astype(jnp.int32)
    owners_keys = jax.random.split(jax.random.fold_in(key_list[2], 1), TILES // TILES_DEV)
    owners_turns = jax.random.permutation(jax.random.fold_in(key_list[2], 3), TILES // TILES_DEV)
    owners = jax.vmap(lambda own, number: assign_block(jax.random.fold_in(key_list[2], 2), own, number, TILES_DEV, N_SHUF, 1, CAP, 1))(owners_keys, owners_turns).reshape((TILES, 1))
    col_gain = jnp.clip(1.0 + 0.1 * jax.random.normal(key_list[3], (COLS,), jnp.float32), 0.5, 1.5)
    col_bias = normal_values(key_list[4], (COLS,), 0.5, 3.0, ((0, 4),), jnp.float32)
    out_weight = normal_values(key_list[5], (COLS, OUT), COLS ** -0.5, 0.1875, ((0, 4),))
    return {"values": values, "subgroup": subgroup, "owners": owners, "col_gain": col_gain, "col_bias": col_bias, "out_weight": out_weight}


def reference(values, subgroup, owners, col_gain, col_bias, out_weight):
    row_total, col_total = values.shape
    tile_total = row_total // TILE
    groups = GRP_DEV * N_SHUF
    group = (owners[:, 0] * GRP_DEV + subgroup).astype(jnp.int32)
    shaped = values.astype(jnp.float32).reshape(tile_total, TILE, col_total)
    tile_sum = lax.optimization_barrier(jnp.sum(shaped, axis=1))
    tile_sq = lax.optimization_barrier(jnp.sum(shaped * shaped, axis=1))
    group_sum = jax.ops.segment_sum(tile_sum, group, num_segments=groups)
    group_sq = jax.ops.segment_sum(tile_sq, group, num_segments=groups)
    count = jax.ops.segment_sum(jnp.full((tile_total,), float(TILE), jnp.float32), group, num_segments=groups)
    mean_all = lax.optimization_barrier(jnp.sum(tile_sum, axis=0)) / float(row_total)
    square_all = lax.optimization_barrier(jnp.sum(tile_sq, axis=0)) / float(row_total)
    weight = (count + float(PRIOR))[:, None]
    center = (group_sum + float(PRIOR) * mean_all) / weight
    second = (group_sq + float(PRIOR) * square_all) / weight
    inverse = lax.rsqrt(second - center * center + 1e-05)
    tile_center = center[group]
    tile_scale = inverse[group] * col_gain
    scored = ((shaped - tile_center[:, None, :]) * tile_scale[:, None, :] + col_bias).astype(jnp.bfloat16)
    scored = scored.reshape(row_total, col_total)
    block_cols = col_total // N_REP
    summed = jnp.zeros((row_total, out_weight.shape[1]), jnp.float32)
    for block in range(N_REP):
        partial_value = jnp.dot(scored[:, block * block_cols:(block + 1) * block_cols], out_weight[block * block_cols:(block + 1) * block_cols], preferred_element_type=jnp.float32)
        summed = summed + partial_value.astype(jnp.bfloat16).astype(jnp.float32)
    return summed.astype(jnp.bfloat16)
```

```python
import functools
import math

import jax
import jax.numpy as jnp
from jax import lax
from jax.experimental import pallas as pl
from jax.experimental.pallas import tpu as pltpu
from jax.sharding import PartitionSpec as P

GRP_DEV = 32
PRIOR = 256
EPS = 1e-05
EXTRA = 8
CHUNKS = 8
FIRST = 5
LOADS = 8
MESH = pl.DeviceIdType.MESH


def kernel(
    shuf_size,
    rep_size,
    values,
    weight,
    gid_cols,
    gid_rows,
    gain,
    bias,
    out,
    held,
    arrived,
    packets,
    weights,
    stats_out,
    stats_in,
    scored,
    load_sem,
    own_sem,
    val_send,
    val_recv,
    pack_send,
    pack_recv,
    fwd_send,
    fwd_recv,
    wx_send,
    wx_recv,
    wg_send,
    wg_recv,
    wf_send,
    wf_recv,
    wn_send,
    wn_recv,
    st_send,
    st_recv,
):
    shuf, rep = lax.axis_index("shuf"), lax.axis_index("rep")
    half = rep_size // 2
    outer = shuf_size // 2
    slices = weights.shape[2]
    slice_outer = slices // 2
    local_rows, cols = values.shape
    block_rows = local_rows // rep_size
    tiles = gid_cols.shape[0] - EXTRA
    tile_rows = local_rows // tiles
    block_tiles = tiles // rep_size
    chunk = block_rows // CHUNKS
    high, low = rep // half, rep % half
    s_out, s_in = shuf // 2, shuf % 2
    mate = s_out * 2 + 1 - s_in
    cut = shuf % slices
    cut_base = shuf - cut
    cut_out = cut // 2

    def rep_peer(dh, dl):
        return ((high + dh) % 2) * half + (low + dl) % half

    def outer_peer(e):
        return ((s_out + e) % outer) * 2 + s_in

    def cut_peer(e):
        return cut_base + ((cut_out + e) % slice_outer) * 2 + s_in

    rep_offsets = [(dh, dl) for dh in range(2) for dl in range(half) if (dh, dl) != (0, 0)]

    def remote(src, dst, send, recv, s, k):
        return pltpu.make_async_remote_copy(
            src_ref=src, dst_ref=dst, send_sem=send, recv_sem=recv,
            device_id=(s, k), device_id_type=MESH,
        )

    def value_copy(dh, dl, ch):
        peer = rep_peer(dh, dl)
        slot = dh * half + dl
        start = pl.multiple_of(peer * block_rows + ch * chunk, chunk)
        return remote(
            values.at[pl.ds(start, chunk)],
            arrived.at[slot, pl.ds(ch * chunk, chunk)],
            val_send.at[slot, ch], val_recv.at[slot, ch], shuf, peer,
        )

    def load_copy(i):
        size = local_rows // LOADS
        return pltpu.make_async_copy(
            values.at[pl.ds(i * size, size)], held.at[pl.ds(i * size, size)], load_sem.at[i]
        )

    own_weight = pltpu.make_async_copy(weight, weights.at[0, 0], own_sem)
    for i in range(LOADS):
        load_copy(i).start()
    own_weight.start()

    barrier = pltpu.get_barrier_semaphore()
    peers = [(shuf, rep_peer(dh, dl)) for dh, dl in rep_offsets]
    peers += [(mate, rep)] + [(outer_peer(e), rep) for e in range(1, outer)]
    for s, k in peers:
        pl.semaphore_signal(barrier, inc=1, device_id=(s, k), device_id_type=MESH)
    pl.semaphore_wait(barrier, len(peers))

    wx = remote(weight.at[cut], weights.at[1, 0, cut], wx_send, wx_recv, shuf, rep_peer(1, 0))
    wx.start()
    far = [(1, dl) for dl in range(half)]
    near = [(0, dl) for dl in range(1, half)]
    for ch in range(FIRST):
        for dh, dl in far:
            value_copy(dh, dl, ch).start()
    for ch in range(CHUNKS):
        for dh, dl in near:
            value_copy(dh, dl, ch).start()

    packets[0, 0, tiles:, :] = gid_rows[...]
    group = 8
    per_load = tiles // LOADS
    for i in range(LOADS):
        load_copy(i).wait()

        def sums(g, carry):
            first = pl.multiple_of(i * per_load + g * group, group)
            parts, squares = [], []
            for u in range(group):
                x = held[pl.ds(pl.multiple_of((first + u) * tile_rows, tile_rows), tile_rows), :]
                x = x.astype(jnp.float32)
                parts.append(jnp.sum(x, axis=0, keepdims=True))
                squares.append(jnp.sum(x * x, axis=0, keepdims=True))
            packets[0, 0, pl.ds(first, group), :cols] = jnp.concatenate(parts, axis=0)
            packets[0, 0, pl.ds(first, group), cols:] = jnp.concatenate(squares, axis=0)
            return carry

        lax.fori_loop(0, per_load // group, sums, 0)

    def pack_copy(e):
        return remote(
            packets.at[0, 0], packets.at[0, e], pack_send.at[e], pack_recv.at[e], outer_peer(e), rep
        )

    def fwd_copy(e):
        return remote(
            packets.at[0, e], packets.at[1, e], fwd_send.at[e], fwd_recv.at[e], mate, rep
        )

    def cut_copy(e):
        here = weights.at[1, 0, cut]
        return remote(here, here, wg_send.at[e], wg_recv.at[e], cut_peer(e), rep)

    def cut_forward(e):
        index = ((cut_out + slice_outer - e) % slice_outer) * 2 + s_in
        there = weights.at[1, 0, index]
        return remote(there, there, wf_send.at[e], wf_recv.at[e], mate, rep)

    for e in range(1, outer):
        pack_copy(e).start()
    fwd_copy(0).start()
    wx.wait_recv()
    for e in range(1, slice_outer):
        cut_copy(e).start()

    def members(i, e):
        same = gid_cols[...] == packets[i, e, tiles:tiles + 1, :tiles]
        row = lax.broadcasted_iota(jnp.int32, (tiles + EXTRA, tiles), 0)
        return jnp.where(same | (row >= tiles), 1.0, 0.0).astype(jnp.float32)

    def gathered(i, e):
        m = members(i, e)
        part = jnp.dot(
            m, packets[i, e, :tiles, :],
            precision=lax.Precision.HIGHEST, preferred_element_type=jnp.float32,
        )
        return part, jnp.sum(m, axis=1, keepdims=True)

    total, count = gathered(0, 0)
    for e in range(1, outer):
        pack_copy(e).wait_recv()
        fwd_copy(e).start()
        part, number = gathered(0, e)
        total, count = total + part, count + number
    cut_forward(0).start()
    for e in range(1, slice_outer):
        cut_copy(e).wait_recv()
        cut_forward(e).start()
    for e in range(outer):
        fwd_copy(e).wait_recv()
        part, number = gathered(1, e)
        total, count = total + part, count + number

    row_count = float(local_rows * shuf_size)
    overall = total[tiles:tiles + 1] / row_count
    weight_sum = count[:tiles] * float(tile_rows) + float(PRIOR)
    pooled = (total[:tiles] + float(PRIOR) * overall) / weight_sum
    center, second = pooled[:, :cols], pooled[:, cols:]
    scale = lax.rsqrt(second - center * center + EPS) * gain[...]
    offset = bias[...] - center * scale
    for j in range(rep_size):
        stats_out[j, 0] = scale[j * block_tiles:(j + 1) * block_tiles]
        stats_out[j, 1] = offset[j * block_tiles:(j + 1) * block_tiles]

    def stat_copy(dh, dl):
        peer = rep_peer(dh, dl)
        slot = dh * half + dl
        return remote(
            stats_out.at[peer], stats_in.at[slot], st_send.at[slot], st_recv.at[slot], shuf, peer
        )

    for dh, dl in reversed(rep_offsets):
        stat_copy(dh, dl).start()
    for ch in range(FIRST, CHUNKS):
        for dh, dl in far:
            value_copy(dh, dl, ch).start()
    stats_in[0] = stats_out[rep]

    own_weight.wait()
    for e in range(slice_outer):
        cut_forward(e).wait_recv()

    def near_copy(dh, dl):
        return remote(
            weights.at[dh, 0], weights.at[dh, dl],
            wn_send.at[dh, dl], wn_recv.at[dh, dl], shuf, rep_peer(0, dl),
        )

    for dl in range(1, half):
        for dh in range(2):
            near_copy(dh, dl).start()
    for dh, dl in rep_offsets:
        stat_copy(dh, dl).wait_recv()
    for dl in range(1, half):
        for dh in range(2):
            near_copy(dh, dl).wait_recv()

    def project(ch, carry):
        for dh, dl in rep_offsets:
            value_copy(dh, dl, ch).wait_recv()
        for slot in range(rep_size):
            for u in range(chunk // tile_rows):
                tile = ch * (chunk // tile_rows) + u
                at = ch * chunk + u * tile_rows
                if slot == 0:
                    start = pl.multiple_of(rep * block_rows + at, tile_rows)
                    x = held[pl.ds(start, tile_rows), :]
                else:
                    x = arrived[slot, pl.ds(pl.multiple_of(at, tile_rows), tile_rows), :]
                s = stats_in[slot, 0, pl.ds(tile, 1), :]
                t = stats_in[slot, 1, pl.ds(tile, 1), :]
                scored[u * tile_rows:(u + 1) * tile_rows, slot * cols:(slot + 1) * cols] = (
                    x.astype(jnp.float32) * s + t
                ).astype(jnp.bfloat16)
        whole = weights[...].reshape(rep_size * cols, weights.shape[-1])
        out[pl.ds(pl.multiple_of(ch * chunk, chunk), chunk), :] = jnp.dot(
            scored[...], whole, preferred_element_type=jnp.float32
        ).astype(out.dtype)
        return carry

    lax.fori_loop(0, CHUNKS, project, 0)

    wx.wait_send()
    for ch in range(CHUNKS):
        for dh, dl in rep_offsets:
            value_copy(dh, dl, ch).wait_send()
    for e in range(1, outer):
        pack_copy(e).wait_send()
    for e in range(outer):
        fwd_copy(e).wait_send()
    for e in range(1, slice_outer):
        cut_copy(e).wait_send()
    for e in range(slice_outer):
        cut_forward(e).wait_send()
    for dh, dl in rep_offsets:
        stat_copy(dh, dl).wait_send()
    for dl in range(1, half):
        for dh in range(2):
            near_copy(dh, dl).wait_send()


def on_device(shuf_size, rep_size, values, subgroup, owners, col_gain, col_bias, out_weight):
    local_rows, cols = values.shape
    tiles = subgroup.shape[0]
    outs = out_weight.shape[1]
    group = (owners[:, 0] * GRP_DEV + subgroup).astype(jnp.float32)
    gid_cols = jnp.broadcast_to(
        jnp.pad(group, (0, EXTRA), constant_values=-1.0)[:, None], (tiles + EXTRA, tiles)
    )
    gid_rows = jnp.broadcast_to(
        jnp.pad(group, (0, 2 * cols - tiles), constant_values=-2.0)[None, :], (EXTRA, 2 * cols)
    )
    slices = math.gcd(shuf_size, cols // 32)
    outer, half, slice_outer = shuf_size // 2, rep_size // 2, slices // 2
    block_rows = local_rows // rep_size
    chunk = block_rows // CHUNKS
    f32, bf16 = jnp.float32, jnp.bfloat16
    dma = pltpu.SemaphoreType.DMA
    vmem = pl.BlockSpec(memory_space=pltpu.VMEM)
    anywhere = pl.BlockSpec(memory_space=pl.ANY)
    return pl.pallas_call(
        functools.partial(kernel, shuf_size, rep_size),
        out_shape=jax.ShapeDtypeStruct((block_rows, outs), bf16),
        in_specs=[anywhere, anywhere, vmem, vmem, vmem, vmem],
        out_specs=vmem,
        scratch_shapes=[
            pltpu.VMEM((local_rows, cols), bf16),
            pltpu.VMEM((rep_size, block_rows, cols), bf16),
            pltpu.VMEM((2, outer, tiles + EXTRA, 2 * cols), f32),
            pltpu.VMEM((2, half, slices, cols // slices, outs), bf16),
            pltpu.VMEM((rep_size, 2, tiles // rep_size, cols), f32),
            pltpu.VMEM((rep_size, 2, tiles // rep_size, cols), f32),
            pltpu.VMEM((chunk, rep_size * cols), bf16),
            dma((LOADS,)),
            dma,
            dma((rep_size, CHUNKS)),
            dma((rep_size, CHUNKS)),
            dma((outer,)),
            dma((outer,)),
            dma((outer,)),
            dma((outer,)),
            dma,
            dma,
            dma((slice_outer,)),
            dma((slice_outer,)),
            dma((slice_outer,)),
            dma((slice_outer,)),
            dma((2, half)),
            dma((2, half)),
            dma((rep_size,)),
            dma((rep_size,)),
        ],
        compiler_params=pltpu.CompilerParams(collective_id=0, has_side_effects=True),
    )(
        values,
        out_weight.reshape(slices, cols // slices, outs),
        gid_cols,
        gid_rows,
        col_gain[None, :],
        col_bias[None, :],
    )


def solution(mesh):
    return jax.shard_map(
        functools.partial(on_device, mesh.shape["shuf"], mesh.shape["rep"]),
        mesh=mesh,
        in_specs=(P("shuf", "rep"), P("shuf"), P("shuf", None), P("rep"), P("rep"), P("rep", None)),
        out_specs=P(("shuf", "rep"), None),
        check_vma=False,
    )
```

```python
import functools
import math

import jax
import jax.numpy as jnp
from jax import lax
from jax.experimental import pallas as pl
from jax.experimental.pallas import tpu as pltpu
from jax.sharding import PartitionSpec as P

GRP_DEV = 32
PRIOR = 256
EPS = 1e-05
EXTRA = 8
CHUNKS = 8
FIRST = 5
LOADS = 8
LIMIT = 59 * 1024 * 1024
MESH = pl.DeviceIdType.MESH


def kernel(
    shuf_size,
    rep_size,
    values,
    weight,
    owner,
    member,
    gain,
    bias,
    out,
    held,
    arrived,
    packets,
    weights,
    stats_out,
    stats_in,
    scored,
    load_sem,
    own_sem,
    val_send,
    val_recv,
    pack_send,
    pack_recv,
    fwd_send,
    fwd_recv,
    wx_send,
    wx_recv,
    wg_send,
    wg_recv,
    wf_send,
    wf_recv,
    wn_send,
    wn_recv,
    st_send,
    st_recv,
):
    shuf, rep = lax.axis_index("shuf"), lax.axis_index("rep")
    half = rep_size // 2
    outer = shuf_size // 2
    slices = weights.shape[2]
    slice_outer = slices // 2
    local_rows, cols = values.shape
    block_rows = local_rows // rep_size
    tiles = member.shape[1]
    tile_rows = local_rows // tiles
    block_tiles = tiles // rep_size
    chunk = block_rows // CHUNKS
    high, low = rep // half, rep % half
    s_out, s_in = shuf // 2, shuf % 2
    mate = s_out * 2 + 1 - s_in
    cut = shuf % slices
    cut_base = shuf - cut
    cut_out = cut // 2

    def rep_peer(dh, dl):
        return ((high + dh) % 2) * half + (low + dl) % half

    def outer_peer(e):
        return ((s_out + e) % outer) * 2 + s_in

    def cut_peer(e):
        return cut_base + ((cut_out + e) % slice_outer) * 2 + s_in

    rep_offsets = [(dh, dl) for dh in range(2) for dl in range(half) if (dh, dl) != (0, 0)]

    def remote(src, dst, send, recv, s, k):
        return pltpu.make_async_remote_copy(
            src_ref=src, dst_ref=dst, send_sem=send, recv_sem=recv,
            device_id=(s, k), device_id_type=MESH,
        )

    def value_copy(dh, dl, ch):
        peer = rep_peer(dh, dl)
        slot = dh * half + dl
        start = pl.multiple_of(peer * block_rows + ch * chunk, chunk)
        return remote(
            values.at[pl.ds(start, chunk)],
            arrived.at[slot, pl.ds(ch * chunk, chunk)],
            val_send.at[slot, ch], val_recv.at[slot, ch], shuf, peer,
        )

    def load_copy(i):
        size = local_rows // LOADS
        return pltpu.make_async_copy(
            values.at[pl.ds(i * size, size)], held.at[pl.ds(i * size, size)], load_sem.at[i]
        )

    own_weight = pltpu.make_async_copy(weight, weights.at[0, 0], own_sem)
    for i in range(LOADS):
        load_copy(i).start()
    own_weight.start()

    barrier = pltpu.get_barrier_semaphore()
    peers = [(shuf, rep_peer(dh, dl)) for dh, dl in rep_offsets]
    peers += [(mate, rep)] + [(outer_peer(e), rep) for e in range(1, outer)]
    for s, k in peers:
        pl.semaphore_signal(barrier, inc=1, device_id=(s, k), device_id_type=MESH)
    pl.semaphore_wait(barrier, len(peers))

    wx = remote(weight.at[cut], weights.at[1, 0, cut], wx_send, wx_recv, shuf, rep_peer(1, 0))
    wx.start()
    far = [(1, dl) for dl in range(half)]
    near = [(0, dl) for dl in range(1, half)]
    for ch in range(FIRST):
        for dh, dl in far:
            value_copy(dh, dl, ch).start()
    for ch in range(CHUNKS):
        for dh, dl in near:
            value_copy(dh, dl, ch).start()

    gid_row = (owner[...] * GRP_DEV + member[...]).astype(jnp.float32)
    packets[0, 0, tiles:tiles + 1, :tiles] = gid_row
    square = (tiles, tiles)
    on_diagonal = lax.broadcasted_iota(jnp.int32, square, 0) == lax.broadcasted_iota(jnp.int32, square, 1)
    gid_col = jnp.sum(jnp.where(on_diagonal, gid_row, 0.0), axis=1, keepdims=True)
    gid_col = jnp.concatenate([gid_col, jnp.full((EXTRA, 1), -1.0, jnp.float32)], axis=0)
    group = 8
    per_load = tiles // LOADS
    for i in range(LOADS):
        load_copy(i).wait()

        def sums(g, carry):
            first = pl.multiple_of(i * per_load + g * group, group)
            parts, squares = [], []
            for u in range(group):
                x = held[pl.ds(pl.multiple_of((first + u) * tile_rows, tile_rows), tile_rows), :]
                x = x.astype(jnp.float32)
                parts.append(jnp.sum(x, axis=0, keepdims=True))
                squares.append(jnp.sum(x * x, axis=0, keepdims=True))
            packets[0, 0, pl.ds(first, group), :cols] = jnp.concatenate(parts, axis=0)
            packets[0, 0, pl.ds(first, group), cols:] = jnp.concatenate(squares, axis=0)
            return carry

        lax.fori_loop(0, per_load // group, sums, 0)

    def pack_copy(e):
        return remote(
            packets.at[0, 0], packets.at[0, e], pack_send.at[e], pack_recv.at[e], outer_peer(e), rep
        )

    def fwd_copy(e):
        return remote(
            packets.at[0, e], packets.at[1, e], fwd_send.at[e], fwd_recv.at[e], mate, rep
        )

    def cut_copy(e):
        here = weights.at[1, 0, cut]
        return remote(here, here, wg_send.at[e], wg_recv.at[e], cut_peer(e), rep)

    def cut_forward(e):
        index = ((cut_out + slice_outer - e) % slice_outer) * 2 + s_in
        there = weights.at[1, 0, index]
        return remote(there, there, wf_send.at[e], wf_recv.at[e], mate, rep)

    for e in range(1, outer):
        pack_copy(e).start()
    fwd_copy(0).start()
    wx.wait_recv()
    for e in range(1, slice_outer):
        cut_copy(e).start()

    def members(i, e):
        same = gid_col == packets[i, e, tiles:tiles + 1, :tiles]
        row = lax.broadcasted_iota(jnp.int32, (tiles + EXTRA, tiles), 0)
        return jnp.where(same | (row >= tiles), 1.0, 0.0).astype(jnp.float32)

    def gathered(i, e):
        m = members(i, e)
        part = jnp.dot(
            m, packets[i, e, :tiles, :],
            precision=lax.Precision.HIGHEST, preferred_element_type=jnp.float32,
        )
        return part, jnp.sum(m, axis=1, keepdims=True)

    total, count = gathered(0, 0)
    for e in range(1, outer):
        pack_copy(e).wait_recv()
        fwd_copy(e).start()
        part, number = gathered(0, e)
        total, count = total + part, count + number
    cut_forward(0).start()
    for e in range(1, slice_outer):
        cut_copy(e).wait_recv()
        cut_forward(e).start()
    for e in range(outer):
        fwd_copy(e).wait_recv()
        part, number = gathered(1, e)
        total, count = total + part, count + number

    row_count = float(local_rows * shuf_size)
    overall = total[tiles:tiles + 1] / row_count
    weight_sum = count[:tiles] * float(tile_rows) + float(PRIOR)
    pooled = (total[:tiles] + float(PRIOR) * overall) / weight_sum
    center, second = pooled[:, :cols], pooled[:, cols:]
    scale = lax.rsqrt(second - center * center + EPS) * gain[...]
    offset = bias[...] - center * scale
    for j in range(rep_size):
        stats_out[j, 0] = scale[j * block_tiles:(j + 1) * block_tiles]
        stats_out[j, 1] = offset[j * block_tiles:(j + 1) * block_tiles]

    def stat_copy(dh, dl):
        peer = rep_peer(dh, dl)
        slot = dh * half + dl
        return remote(
            stats_out.at[peer], stats_in.at[slot], st_send.at[slot], st_recv.at[slot], shuf, peer
        )

    for dh, dl in reversed(rep_offsets):
        stat_copy(dh, dl).start()
    for ch in range(FIRST, CHUNKS):
        for dh, dl in far:
            value_copy(dh, dl, ch).start()
    stats_in[0] = stats_out[rep]

    own_weight.wait()
    for e in range(slice_outer):
        cut_forward(e).wait_recv()

    def near_copy(dh, dl):
        return remote(
            weights.at[dh, 0], weights.at[dh, dl],
            wn_send.at[dh, dl], wn_recv.at[dh, dl], shuf, rep_peer(0, dl),
        )

    for dl in range(1, half):
        for dh in range(2):
            near_copy(dh, dl).start()
    for dh, dl in rep_offsets:
        stat_copy(dh, dl).wait_recv()
    for dl in range(1, half):
        for dh in range(2):
            near_copy(dh, dl).wait_recv()

    def project(ch, carry):
        for dh, dl in rep_offsets:
            value_copy(dh, dl, ch).wait_recv()
        for slot in range(rep_size):
            for u in range(chunk // tile_rows):
                tile = ch * (chunk // tile_rows) + u
                at = ch * chunk + u * tile_rows
                if slot == 0:
                    start = pl.multiple_of(rep * block_rows + at, tile_rows)
                    x = held[pl.ds(start, tile_rows), :]
                else:
                    x = arrived[slot, pl.ds(pl.multiple_of(at, tile_rows), tile_rows), :]
                s = stats_in[slot, 0, pl.ds(tile, 1), :]
                t = stats_in[slot, 1, pl.ds(tile, 1), :]
                scored[u * tile_rows:(u + 1) * tile_rows, slot * cols:(slot + 1) * cols] = (
                    x.astype(jnp.float32) * s + t
                ).astype(jnp.bfloat16)
        whole = weights[...].reshape(rep_size * cols, weights.shape[-1])
        out[pl.ds(pl.multiple_of(ch * chunk, chunk), chunk), :] = jnp.dot(
            scored[...], whole, preferred_element_type=jnp.float32
        ).astype(out.dtype)
        return carry

    lax.fori_loop(0, CHUNKS, project, 0)

    wx.wait_send()
    for ch in range(CHUNKS):
        for dh, dl in rep_offsets:
            value_copy(dh, dl, ch).wait_send()
    for e in range(1, outer):
        pack_copy(e).wait_send()
    for e in range(outer):
        fwd_copy(e).wait_send()
    for e in range(1, slice_outer):
        cut_copy(e).wait_send()
    for e in range(slice_outer):
        cut_forward(e).wait_send()
    for dh, dl in rep_offsets:
        stat_copy(dh, dl).wait_send()
    for dl in range(1, half):
        for dh in range(2):
            near_copy(dh, dl).wait_send()


def on_device(shuf_size, rep_size, values, subgroup, owners, col_gain, col_bias, out_weight):
    local_rows, cols = values.shape
    tiles = subgroup.shape[0]
    outs = out_weight.shape[1]
    slices = math.gcd(shuf_size, cols // 32)
    outer, half, slice_outer = shuf_size // 2, rep_size // 2, slices // 2
    block_rows = local_rows // rep_size
    chunk = block_rows // CHUNKS
    f32, bf16 = jnp.float32, jnp.bfloat16
    dma = pltpu.SemaphoreType.DMA
    vmem = pl.BlockSpec(memory_space=pltpu.VMEM)
    hbm = pl.BlockSpec(memory_space=pltpu.HBM)
    return pl.pallas_call(
        functools.partial(kernel, shuf_size, rep_size),
        out_shape=pltpu.VMEM((block_rows, outs), bf16),
        in_specs=[hbm, hbm, vmem, vmem, vmem, vmem],
        out_specs=vmem,
        scratch_shapes=[
            pltpu.VMEM((local_rows, cols), bf16),
            pltpu.VMEM((rep_size, block_rows, cols), bf16),
            pltpu.VMEM((2, outer, tiles + EXTRA, 2 * cols), f32),
            pltpu.VMEM((2, half, slices, cols // slices, outs), bf16),
            pltpu.VMEM((rep_size, 2, tiles // rep_size, cols), f32),
            pltpu.VMEM((rep_size, 2, tiles // rep_size, cols), f32),
            pltpu.VMEM((chunk, rep_size * cols), bf16),
            dma((LOADS,)),
            dma,
            dma((rep_size, CHUNKS)),
            dma((rep_size, CHUNKS)),
            dma((outer,)),
            dma((outer,)),
            dma((outer,)),
            dma((outer,)),
            dma,
            dma,
            dma((slice_outer,)),
            dma((slice_outer,)),
            dma((slice_outer,)),
            dma((slice_outer,)),
            dma((2, half)),
            dma((2, half)),
            dma((rep_size,)),
            dma((rep_size,)),
        ],
        compiler_params=pltpu.CompilerParams(
            collective_id=0, has_side_effects=True, vmem_limit_bytes=LIMIT
        ),
    )(
        values,
        out_weight.reshape(slices, cols // slices, outs),
        owners.reshape(1, tiles),
        subgroup.reshape(1, tiles),
        col_gain[None, :],
        col_bias[None, :],
    )


def solution(mesh):
    return jax.shard_map(
        functools.partial(on_device, mesh.shape["shuf"], mesh.shape["rep"]),
        mesh=mesh,
        in_specs=(P("shuf", "rep"), P("shuf"), P("shuf", None), P("rep"), P("rep"), P("rep", None)),
        out_specs=P(("shuf", "rep"), None),
        check_vma=False,
    )
```

```python
import functools
import math

import jax
import jax.numpy as jnp
from jax import lax
from jax.experimental import pallas as pl
from jax.experimental.pallas import tpu as pltpu
from jax.sharding import PartitionSpec as P

GRP_DEV = 32
PRIOR = 256
EPS = 1e-05
EXTRA = 8
CHUNKS = 8
FIRST = 5
LOADS = 8
LIMIT = 58900 * 1024
LIMIT_LAST = 8 * 1024 * 1024
MESH = pl.DeviceIdType.MESH


def kernel(
    shuf_size,
    rep_size,
    values,
    weight,
    owner,
    member,
    gain,
    bias,
    out,
    last_scored,
    weights,
    held,
    arrived,
    packets,
    stats_out,
    stats_in,
    scored,
    load_sem,
    own_sem,
    val_send,
    val_recv,
    pack_send,
    pack_recv,
    fwd_send,
    fwd_recv,
    wx_send,
    wx_recv,
    wg_send,
    wg_recv,
    wf_send,
    wf_recv,
    wn_send,
    wn_recv,
    st_send,
    st_recv,
):
    shuf, rep = lax.axis_index("shuf"), lax.axis_index("rep")
    half = rep_size // 2
    outer = shuf_size // 2
    slices = weights.shape[2]
    slice_outer = slices // 2
    local_rows, cols = values.shape
    block_rows = local_rows // rep_size
    tiles = member.shape[1]
    tile_rows = local_rows // tiles
    block_tiles = tiles // rep_size
    chunk = block_rows // CHUNKS
    high, low = rep // half, rep % half
    s_out, s_in = shuf // 2, shuf % 2
    mate = s_out * 2 + 1 - s_in
    cut = shuf % slices
    cut_base = shuf - cut
    cut_out = cut // 2

    def rep_peer(dh, dl):
        return ((high + dh) % 2) * half + (low + dl) % half

    def outer_peer(e):
        return ((s_out + e) % outer) * 2 + s_in

    def cut_peer(e):
        return cut_base + ((cut_out + e) % slice_outer) * 2 + s_in

    rep_offsets = [(dh, dl) for dh in range(2) for dl in range(half) if (dh, dl) != (0, 0)]

    def remote(src, dst, send, recv, s, k):
        return pltpu.make_async_remote_copy(
            src_ref=src, dst_ref=dst, send_sem=send, recv_sem=recv,
            device_id=(s, k), device_id_type=MESH,
        )

    def value_copy(dh, dl, ch):
        peer = rep_peer(dh, dl)
        slot = dh * half + dl
        start = pl.multiple_of(peer * block_rows + ch * chunk, chunk)
        return remote(
            values.at[pl.ds(start, chunk)],
            arrived.at[slot, pl.ds(ch * chunk, chunk)],
            val_send.at[slot, ch], val_recv.at[slot, ch], shuf, peer,
        )

    def load_copy(i):
        size = local_rows // LOADS
        return pltpu.make_async_copy(
            values.at[pl.ds(i * size, size)], held.at[pl.ds(i * size, size)], load_sem.at[i]
        )

    own_weight = pltpu.make_async_copy(weight, weights.at[0, 0], own_sem)
    for i in range(LOADS):
        load_copy(i).start()
    own_weight.start()

    barrier = pltpu.get_barrier_semaphore()
    peers = [(shuf, rep_peer(dh, dl)) for dh, dl in rep_offsets]
    peers += [(mate, rep)] + [(outer_peer(e), rep) for e in range(1, outer)]
    for s, k in peers:
        pl.semaphore_signal(barrier, inc=1, device_id=(s, k), device_id_type=MESH)
    pl.semaphore_wait(barrier, len(peers))

    wx = remote(weight.at[cut], weights.at[1, 0, cut], wx_send, wx_recv, shuf, rep_peer(1, 0))
    wx.start()
    far = [(1, dl) for dl in range(half)]
    near = [(0, dl) for dl in range(1, half)]
    for ch in range(FIRST):
        for dh, dl in far:
            value_copy(dh, dl, ch).start()
    for ch in range(CHUNKS):
        for dh, dl in near:
            value_copy(dh, dl, ch).start()

    gid_row = (owner[...] * GRP_DEV + member[...]).astype(jnp.float32)
    packets[0, 0, tiles:tiles + 1, :tiles] = gid_row
    square = (tiles, tiles)
    on_diagonal = lax.broadcasted_iota(jnp.int32, square, 0) == lax.broadcasted_iota(jnp.int32, square, 1)
    gid_col = jnp.sum(jnp.where(on_diagonal, gid_row, 0.0), axis=1, keepdims=True)
    gid_col = jnp.concatenate([gid_col, jnp.full((EXTRA, 1), -1.0, jnp.float32)], axis=0)
    group = 8
    per_load = tiles // LOADS
    for i in range(LOADS):
        load_copy(i).wait()

        def sums(g, carry):
            first = pl.multiple_of(i * per_load + g * group, group)
            parts, squares = [], []
            for u in range(group):
                x = held[pl.ds(pl.multiple_of((first + u) * tile_rows, tile_rows), tile_rows), :]
                x = x.astype(jnp.float32)
                parts.append(jnp.sum(x, axis=0, keepdims=True))
                squares.append(jnp.sum(x * x, axis=0, keepdims=True))
            packets[0, 0, pl.ds(first, group), :cols] = jnp.concatenate(parts, axis=0)
            packets[0, 0, pl.ds(first, group), cols:] = jnp.concatenate(squares, axis=0)
            return carry

        lax.fori_loop(0, per_load // group, sums, 0)

    def pack_copy(e):
        return remote(
            packets.at[0, 0], packets.at[0, e], pack_send.at[e], pack_recv.at[e], outer_peer(e), rep
        )

    def fwd_copy(e):
        return remote(
            packets.at[0, e], packets.at[1, e], fwd_send.at[e], fwd_recv.at[e], mate, rep
        )

    def cut_copy(e):
        here = weights.at[1, 0, cut]
        return remote(here, here, wg_send.at[e], wg_recv.at[e], cut_peer(e), rep)

    def cut_forward(e):
        index = ((cut_out + slice_outer - e) % slice_outer) * 2 + s_in
        there = weights.at[1, 0, index]
        return remote(there, there, wf_send.at[e], wf_recv.at[e], mate, rep)

    for e in range(1, outer):
        pack_copy(e).start()
    fwd_copy(0).start()
    wx.wait_recv()
    for e in range(1, slice_outer):
        cut_copy(e).start()

    def members(i, e):
        same = gid_col == packets[i, e, tiles:tiles + 1, :tiles]
        row = lax.broadcasted_iota(jnp.int32, (tiles + EXTRA, tiles), 0)
        return jnp.where(same | (row >= tiles), 1.0, 0.0).astype(jnp.float32)

    def gathered(i, e):
        m = members(i, e)
        part = jnp.dot(
            m, packets[i, e, :tiles, :],
            precision=lax.Precision.HIGHEST, preferred_element_type=jnp.float32,
        )
        return part, jnp.sum(m, axis=1, keepdims=True)

    total, count = gathered(0, 0)
    for e in range(1, outer):
        pack_copy(e).wait_recv()
        fwd_copy(e).start()
        part, number = gathered(0, e)
        total, count = total + part, count + number
    cut_forward(0).start()
    for e in range(1, slice_outer):
        cut_copy(e).wait_recv()
        cut_forward(e).start()
    for e in range(outer):
        fwd_copy(e).wait_recv()
        part, number = gathered(1, e)
        total, count = total + part, count + number

    row_count = float(local_rows * shuf_size)
    overall = total[tiles:tiles + 1] / row_count
    weight_sum = count[:tiles] * float(tile_rows) + float(PRIOR)
    pooled = (total[:tiles] + float(PRIOR) * overall) / weight_sum
    center, second = pooled[:, :cols], pooled[:, cols:]
    scale = lax.rsqrt(second - center * center + EPS) * gain[...]
    offset = bias[...] - center * scale
    for j in range(rep_size):
        stats_out[j, 0] = scale[j * block_tiles:(j + 1) * block_tiles]
        stats_out[j, 1] = offset[j * block_tiles:(j + 1) * block_tiles]

    def stat_copy(dh, dl):
        peer = rep_peer(dh, dl)
        slot = dh * half + dl
        return remote(
            stats_out.at[peer], stats_in.at[slot], st_send.at[slot], st_recv.at[slot], shuf, peer
        )

    for dh, dl in reversed(rep_offsets):
        stat_copy(dh, dl).start()
    for ch in range(FIRST, CHUNKS):
        for dh, dl in far:
            value_copy(dh, dl, ch).start()
    stats_in[0] = stats_out[rep]

    own_weight.wait()
    for e in range(slice_outer):
        cut_forward(e).wait_recv()

    def near_copy(dh, dl):
        return remote(
            weights.at[dh, 0], weights.at[dh, dl],
            wn_send.at[dh, dl], wn_recv.at[dh, dl], shuf, rep_peer(0, dl),
        )

    for dl in range(1, half):
        for dh in range(2):
            near_copy(dh, dl).start()
    for dh, dl in rep_offsets:
        stat_copy(dh, dl).wait_recv()
    for dl in range(1, half):
        for dh in range(2):
            near_copy(dh, dl).wait_recv()

    def score(ch, dst):
        for slot in range(rep_size):
            if slot > 0:
                value_copy(slot // half, slot % half, ch).wait_recv()
            for u in range(chunk // tile_rows):
                tile = ch * (chunk // tile_rows) + u
                at = ch * chunk + u * tile_rows
                if slot == 0:
                    start = pl.multiple_of(rep * block_rows + at, tile_rows)
                    x = held[pl.ds(start, tile_rows), :]
                else:
                    x = arrived[slot, pl.ds(pl.multiple_of(at, tile_rows), tile_rows), :]
                s = stats_in[slot, 0, pl.ds(tile, 1), :]
                t = stats_in[slot, 1, pl.ds(tile, 1), :]
                dst[u * tile_rows:(u + 1) * tile_rows, slot * cols:(slot + 1) * cols] = (
                    x.astype(jnp.float32) * s + t
                ).astype(jnp.bfloat16)

    def project(ch, carry):
        score(ch, scored)
        whole = weights[...].reshape(rep_size * cols, weights.shape[-1])
        out[pl.ds(pl.multiple_of(ch * chunk, chunk), chunk), :] = jnp.dot(
            scored[...], whole, preferred_element_type=jnp.float32
        ).astype(out.dtype)
        return carry

    lax.fori_loop(0, CHUNKS - 1, project, 0)
    score(CHUNKS - 1, last_scored)

    wx.wait_send()
    for ch in range(CHUNKS):
        for dh, dl in rep_offsets:
            value_copy(dh, dl, ch).wait_send()
    for e in range(1, outer):
        pack_copy(e).wait_send()
    for e in range(outer):
        fwd_copy(e).wait_send()
    for e in range(1, slice_outer):
        cut_copy(e).wait_send()
    for e in range(slice_outer):
        cut_forward(e).wait_send()
    for dh, dl in rep_offsets:
        stat_copy(dh, dl).wait_send()
    for dl in range(1, half):
        for dh in range(2):
            near_copy(dh, dl).wait_send()


def finish(early, scored, weights, out, tail, sems):
    rows, last = early.shape[0], scored.shape[0]
    size = rows // (CHUNKS - 1)

    def early_copy(i):
        return pltpu.make_async_copy(
            early.at[pl.ds(i * size, size)], out.at[pl.ds(i * size, size)], sems.at[i]
        )

    for i in range(CHUNKS - 1):
        early_copy(i).start()
    whole = weights[...].reshape(scored.shape[1], weights.shape[-1])
    tail[...] = jnp.dot(scored[...], whole, preferred_element_type=jnp.float32).astype(tail.dtype)
    tail_copy = pltpu.make_async_copy(tail, out.at[pl.ds(rows, last)], sems.at[CHUNKS - 1])
    tail_copy.start()
    for i in range(CHUNKS - 1):
        early_copy(i).wait()
    tail_copy.wait()


def on_device(shuf_size, rep_size, values, subgroup, owners, col_gain, col_bias, out_weight):
    local_rows, cols = values.shape
    tiles = subgroup.shape[0]
    outs = out_weight.shape[1]
    slices = math.gcd(shuf_size, cols // 32)
    outer, half, slice_outer = shuf_size // 2, rep_size // 2, slices // 2
    block_rows = local_rows // rep_size
    chunk = block_rows // CHUNKS
    f32, bf16 = jnp.float32, jnp.bfloat16
    dma = pltpu.SemaphoreType.DMA
    vmem = pl.BlockSpec(memory_space=pltpu.VMEM)
    hbm = pl.BlockSpec(memory_space=pltpu.HBM)
    early, last_scored, weights = pl.pallas_call(
        functools.partial(kernel, shuf_size, rep_size),
        out_shape=(
            pltpu.VMEM((block_rows - chunk, outs), bf16),
            pltpu.VMEM((chunk, rep_size * cols), bf16),
            pltpu.VMEM((2, half, slices, cols // slices, outs), bf16),
        ),
        in_specs=[hbm, hbm, vmem, vmem, vmem, vmem],
        out_specs=(vmem, vmem, vmem),
        scratch_shapes=[
            pltpu.VMEM((local_rows, cols), bf16),
            pltpu.VMEM((rep_size, block_rows, cols), bf16),
            pltpu.VMEM((2, outer, tiles + EXTRA, 2 * cols), f32),
            pltpu.VMEM((rep_size, 2, tiles // rep_size, cols), f32),
            pltpu.VMEM((rep_size, 2, tiles // rep_size, cols), f32),
            pltpu.VMEM((chunk, rep_size * cols), bf16),
            dma((LOADS,)),
            dma,
            dma((rep_size, CHUNKS)),
            dma((rep_size, CHUNKS)),
            dma((outer,)),
            dma((outer,)),
            dma((outer,)),
            dma((outer,)),
            dma,
            dma,
            dma((slice_outer,)),
            dma((slice_outer,)),
            dma((slice_outer,)),
            dma((slice_outer,)),
            dma((2, half)),
            dma((2, half)),
            dma((rep_size,)),
            dma((rep_size,)),
        ],
        compiler_params=pltpu.CompilerParams(
            collective_id=0, has_side_effects=True, vmem_limit_bytes=LIMIT
        ),
    )(
        values,
        out_weight.reshape(slices, cols // slices, outs),
        owners.reshape(1, tiles),
        subgroup.reshape(1, tiles),
        col_gain[None, :],
        col_bias[None, :],
    )
    return pl.pallas_call(
        finish,
        out_shape=jax.ShapeDtypeStruct((block_rows, outs), bf16),
        in_specs=[vmem, vmem, vmem],
        out_specs=hbm,
        scratch_shapes=[pltpu.VMEM((chunk, outs), bf16), dma((CHUNKS,))],
        compiler_params=pltpu.CompilerParams(vmem_limit_bytes=LIMIT_LAST),
    )(early, last_scored, weights)


def solution(mesh):
    return jax.shard_map(
        functools.partial(on_device, mesh.shape["shuf"], mesh.shape["rep"]),
        mesh=mesh,
        in_specs=(P("shuf", "rep"), P("shuf"), P("shuf", None), P("rep"), P("rep"), P("rep", None)),
        out_specs=P(("shuf", "rep"), None),
        check_vma=False,
    )
```

```python
import functools
import math

import jax
import jax.numpy as jnp
from jax import lax
from jax.experimental import pallas as pl
from jax.experimental.pallas import tpu as pltpu
from jax.sharding import PartitionSpec as P

GRP_DEV = 32
PRIOR = 256
EPS = 1e-05
EXTRA = 8
CHUNKS = 8
FIRST = 5
LOADS = 8
LIMIT = 58900 * 1024
LIMIT_LAST = 8 * 1024 * 1024
MESH = pl.DeviceIdType.MESH


def kernel(
    shuf_size,
    rep_size,
    values,
    weight,
    owner,
    member,
    gain,
    bias,
    out,
    last_scored,
    weights,
    held,
    arrived,
    packets,
    stats_out,
    stats_in,
    scored,
    rep_ready,
    shuf_ready,
    load_sem,
    own_sem,
    val_send,
    val_recv,
    pack_send,
    pack_recv,
    fwd_send,
    fwd_recv,
    wx_send,
    wx_recv,
    wg_send,
    wg_recv,
    wf_send,
    wf_recv,
    wn_send,
    wn_recv,
    st_send,
    st_recv,
):
    shuf, rep = lax.axis_index("shuf"), lax.axis_index("rep")
    half = rep_size // 2
    outer = shuf_size // 2
    slices = weights.shape[2]
    slice_outer = slices // 2
    local_rows, cols = values.shape
    block_rows = local_rows // rep_size
    tiles = member.shape[1]
    tile_rows = local_rows // tiles
    block_tiles = tiles // rep_size
    chunk = block_rows // CHUNKS
    high, low = rep // half, rep % half
    s_out, s_in = shuf // 2, shuf % 2
    mate = s_out * 2 + 1 - s_in
    cut = shuf % slices
    cut_base = shuf - cut
    cut_out = cut // 2

    def rep_peer(dh, dl):
        return ((high + dh) % 2) * half + (low + dl) % half

    def outer_peer(e):
        return ((s_out + e) % outer) * 2 + s_in

    def cut_peer(e):
        return cut_base + ((cut_out + e) % slice_outer) * 2 + s_in

    rep_offsets = [(dh, dl) for dh in range(2) for dl in range(half) if (dh, dl) != (0, 0)]

    def remote(src, dst, send, recv, s, k):
        return pltpu.make_async_remote_copy(
            src_ref=src, dst_ref=dst, send_sem=send, recv_sem=recv,
            device_id=(s, k), device_id_type=MESH,
        )

    def value_copy(dh, dl, ch):
        peer = rep_peer(dh, dl)
        slot = dh * half + dl
        start = pl.multiple_of(peer * block_rows + ch * chunk, chunk)
        return remote(
            values.at[pl.ds(start, chunk)],
            arrived.at[slot, pl.ds(ch * chunk, chunk)],
            val_send.at[slot, ch], val_recv.at[slot, ch], shuf, peer,
        )

    def load_copy(i):
        size = local_rows // LOADS
        return pltpu.make_async_copy(
            values.at[pl.ds(i * size, size)], held.at[pl.ds(i * size, size)], load_sem.at[i]
        )

    own_weight = pltpu.make_async_copy(weight, weights.at[0, 0], own_sem)
    for i in range(LOADS):
        load_copy(i).start()
    own_weight.start()

    barrier = pltpu.get_barrier_semaphore()
    leader, scout = low == 0, low == 1
    for dh, dl in rep_offsets:
        peer = rep_peer(dh, dl)

        @pl.when(peer % half == 0)
        def _():
            pl.semaphore_signal(barrier, inc=1, device_id=(shuf, peer), device_id_type=MESH)

    @pl.when(leader)
    def _():
        pl.semaphore_wait(barrier, rep_size - 1)
        for dl in range(1, half):
            pl.semaphore_signal(
                rep_ready, inc=1, device_id=(shuf, rep_peer(0, dl)), device_id_type=MESH
            )

    @pl.when(jnp.logical_not(leader))
    def _():
        pl.semaphore_wait(rep_ready, 1)

    wx = remote(weight.at[cut], weights.at[1, 0, cut], wx_send, wx_recv, shuf, rep_peer(1, 0))
    wx.start()
    far = [(1, dl) for dl in range(half)]
    near = [(0, dl) for dl in range(1, half)]
    for ch in range(FIRST):
        for dh, dl in far:
            value_copy(dh, dl, ch).start()
    for ch in range(CHUNKS):
        for dh, dl in near:
            value_copy(dh, dl, ch).start()

    shuf_peers = [mate] + [outer_peer(e) for e in range(1, outer)]

    @pl.when(scout)
    def _():
        for s in shuf_peers:
            pl.semaphore_signal(barrier, inc=1, device_id=(s, rep), device_id_type=MESH)
        pl.semaphore_wait(barrier, len(shuf_peers))
        for dl in range(1, half):
            pl.semaphore_signal(
                shuf_ready, inc=1, device_id=(shuf, rep_peer(0, dl)), device_id_type=MESH
            )

    @pl.when(jnp.logical_not(scout))
    def _():
        pl.semaphore_wait(shuf_ready, 1)

    gid_row = (owner[...] * GRP_DEV + member[...]).astype(jnp.float32)
    packets[0, 0, tiles:tiles + 1, :tiles] = gid_row
    square = (tiles, tiles)
    on_diagonal = lax.broadcasted_iota(jnp.int32, square, 0) == lax.broadcasted_iota(jnp.int32, square, 1)
    gid_col = jnp.sum(jnp.where(on_diagonal, gid_row, 0.0), axis=1, keepdims=True)
    gid_col = jnp.concatenate([gid_col, jnp.full((EXTRA, 1), -1.0, jnp.float32)], axis=0)
    group = 8
    per_load = tiles // LOADS
    for i in range(LOADS):
        load_copy(i).wait()

        def sums(g, carry):
            first = pl.multiple_of(i * per_load + g * group, group)
            parts, squares = [], []
            for u in range(group):
                x = held[pl.ds(pl.multiple_of((first + u) * tile_rows, tile_rows), tile_rows), :]
                x = x.astype(jnp.float32)
                parts.append(jnp.sum(x, axis=0, keepdims=True))
                squares.append(jnp.sum(x * x, axis=0, keepdims=True))
            packets[0, 0, pl.ds(first, group), :cols] = jnp.concatenate(parts, axis=0)
            packets[0, 0, pl.ds(first, group), cols:] = jnp.concatenate(squares, axis=0)
            return carry

        lax.fori_loop(0, per_load // group, sums, 0)

    def pack_copy(e):
        return remote(
            packets.at[0, 0], packets.at[0, e], pack_send.at[e], pack_recv.at[e], outer_peer(e), rep
        )

    def fwd_copy(e):
        return remote(
            packets.at[0, e], packets.at[1, e], fwd_send.at[e], fwd_recv.at[e], mate, rep
        )

    def cut_copy(e):
        here = weights.at[1, 0, cut]
        return remote(here, here, wg_send.at[e], wg_recv.at[e], cut_peer(e), rep)

    def cut_forward(e):
        index = ((cut_out + slice_outer - e) % slice_outer) * 2 + s_in
        there = weights.at[1, 0, index]
        return remote(there, there, wf_send.at[e], wf_recv.at[e], mate, rep)

    for e in range(1, outer):
        pack_copy(e).start()
    fwd_copy(0).start()
    wx.wait_recv()
    for e in range(1, slice_outer):
        cut_copy(e).start()

    def members(i, e):
        same = gid_col == packets[i, e, tiles:tiles + 1, :tiles]
        row = lax.broadcasted_iota(jnp.int32, (tiles + EXTRA, tiles), 0)
        return jnp.where(same | (row >= tiles), 1.0, 0.0).astype(jnp.float32)

    def gathered(i, e):
        m = members(i, e)
        part = jnp.dot(
            m, packets[i, e, :tiles, :],
            precision=lax.Precision.HIGHEST, preferred_element_type=jnp.float32,
        )
        return part, jnp.sum(m, axis=1, keepdims=True)

    total, count = gathered(0, 0)
    for e in range(1, outer):
        pack_copy(e).wait_recv()
        fwd_copy(e).start()
        part, number = gathered(0, e)
        total, count = total + part, count + number
    cut_forward(0).start()
    for e in range(1, slice_outer):
        cut_copy(e).wait_recv()
        cut_forward(e).start()
    for e in range(outer):
        fwd_copy(e).wait_recv()
        part, number = gathered(1, e)
        total, count = total + part, count + number

    row_count = float(local_rows * shuf_size)
    overall = total[tiles:tiles + 1] / row_count
    weight_sum = count[:tiles] * float(tile_rows) + float(PRIOR)
    pooled = (total[:tiles] + float(PRIOR) * overall) / weight_sum
    center, second = pooled[:, :cols], pooled[:, cols:]
    scale = lax.rsqrt(second - center * center + EPS) * gain[...]
    offset = bias[...] - center * scale
    for j in range(rep_size):
        stats_out[j, 0] = scale[j * block_tiles:(j + 1) * block_tiles]
        stats_out[j, 1] = offset[j * block_tiles:(j + 1) * block_tiles]

    def stat_copy(dh, dl):
        peer = rep_peer(dh, dl)
        slot = dh * half + dl
        return remote(
            stats_out.at[peer], stats_in.at[slot], st_send.at[slot], st_recv.at[slot], shuf, peer
        )

    for dh, dl in reversed(rep_offsets):
        stat_copy(dh, dl).start()
    for ch in range(FIRST, CHUNKS):
        for dh, dl in far:
            value_copy(dh, dl, ch).start()
    stats_in[0] = stats_out[rep]

    own_weight.wait()
    for e in range(slice_outer):
        cut_forward(e).wait_recv()

    def near_copy(dh, dl):
        return remote(
            weights.at[dh, 0], weights.at[dh, dl],
            wn_send.at[dh, dl], wn_recv.at[dh, dl], shuf, rep_peer(0, dl),
        )

    for dl in range(1, half):
        for dh in range(2):
            near_copy(dh, dl).start()
    for dh, dl in rep_offsets:
        stat_copy(dh, dl).wait_recv()
    for dl in range(1, half):
        for dh in range(2):
            near_copy(dh, dl).wait_recv()

    def score(ch, dst):
        for slot in range(rep_size):
            if slot > 0:
                value_copy(slot // half, slot % half, ch).wait_recv()
            for u in range(chunk // tile_rows):
                tile = ch * (chunk // tile_rows) + u
                at = ch * chunk + u * tile_rows
                if slot == 0:
                    start = pl.multiple_of(rep * block_rows + at, tile_rows)
                    x = held[pl.ds(start, tile_rows), :]
                else:
                    x = arrived[slot, pl.ds(pl.multiple_of(at, tile_rows), tile_rows), :]
                s = stats_in[slot, 0, pl.ds(tile, 1), :]
                t = stats_in[slot, 1, pl.ds(tile, 1), :]
                dst[u * tile_rows:(u + 1) * tile_rows, slot * cols:(slot + 1) * cols] = (
                    x.astype(jnp.float32) * s + t
                ).astype(jnp.bfloat16)

    def project(ch, carry):
        score(ch, scored)
        whole = weights[...].reshape(rep_size * cols, weights.shape[-1])
        out[pl.ds(pl.multiple_of(ch * chunk, chunk), chunk), :] = jnp.dot(
            scored[...], whole, preferred_element_type=jnp.float32
        ).astype(out.dtype)
        return carry

    lax.fori_loop(0, CHUNKS - 1, project, 0)
    score(CHUNKS - 1, last_scored)

    wx.wait_send()
    for ch in range(CHUNKS):
        for dh, dl in rep_offsets:
            value_copy(dh, dl, ch).wait_send()
    for e in range(1, outer):
        pack_copy(e).wait_send()
    for e in range(outer):
        fwd_copy(e).wait_send()
    for e in range(1, slice_outer):
        cut_copy(e).wait_send()
    for e in range(slice_outer):
        cut_forward(e).wait_send()
    for dh, dl in rep_offsets:
        stat_copy(dh, dl).wait_send()
    for dl in range(1, half):
        for dh in range(2):
            near_copy(dh, dl).wait_send()


def finish(early, scored, weights, out, tail, sems):
    rows, last = early.shape[0], scored.shape[0]
    size = rows // (CHUNKS - 1)

    def early_copy(i):
        return pltpu.make_async_copy(
            early.at[pl.ds(i * size, size)], out.at[pl.ds(i * size, size)], sems.at[i]
        )

    for i in range(CHUNKS - 1):
        early_copy(i).start()
    whole = weights[...].reshape(scored.shape[1], weights.shape[-1])
    tail[...] = jnp.dot(scored[...], whole, preferred_element_type=jnp.float32).astype(tail.dtype)
    tail_copy = pltpu.make_async_copy(tail, out.at[pl.ds(rows, last)], sems.at[CHUNKS - 1])
    tail_copy.start()
    for i in range(CHUNKS - 1):
        early_copy(i).wait()
    tail_copy.wait()


def on_device(shuf_size, rep_size, values, subgroup, owners, col_gain, col_bias, out_weight):
    local_rows, cols = values.shape
    tiles = subgroup.shape[0]
    outs = out_weight.shape[1]
    slices = math.gcd(shuf_size, cols // 32)
    outer, half, slice_outer = shuf_size // 2, rep_size // 2, slices // 2
    block_rows = local_rows // rep_size
    chunk = block_rows // CHUNKS
    f32, bf16 = jnp.float32, jnp.bfloat16
    dma = pltpu.SemaphoreType.DMA
    vmem = pl.BlockSpec(memory_space=pltpu.VMEM)
    hbm = pl.BlockSpec(memory_space=pltpu.HBM)
    early, last_scored, weights = pl.pallas_call(
        functools.partial(kernel, shuf_size, rep_size),
        out_shape=(
            pltpu.VMEM((block_rows - chunk, outs), bf16),
            pltpu.VMEM((chunk, rep_size * cols), bf16),
            pltpu.VMEM((2, half, slices, cols // slices, outs), bf16),
        ),
        in_specs=[hbm, hbm, vmem, vmem, vmem, vmem],
        out_specs=(vmem, vmem, vmem),
        scratch_shapes=[
            pltpu.VMEM((local_rows, cols), bf16),
            pltpu.VMEM((rep_size, block_rows, cols), bf16),
            pltpu.VMEM((2, outer, tiles + EXTRA, 2 * cols), f32),
            pltpu.VMEM((rep_size, 2, tiles // rep_size, cols), f32),
            pltpu.VMEM((rep_size, 2, tiles // rep_size, cols), f32),
            pltpu.VMEM((chunk, rep_size * cols), bf16),
            pltpu.SemaphoreType.REGULAR,
            pltpu.SemaphoreType.REGULAR,
            dma((LOADS,)),
            dma,
            dma((rep_size, CHUNKS)),
            dma((rep_size, CHUNKS)),
            dma((outer,)),
            dma((outer,)),
            dma((outer,)),
            dma((outer,)),
            dma,
            dma,
            dma((slice_outer,)),
            dma((slice_outer,)),
            dma((slice_outer,)),
            dma((slice_outer,)),
            dma((2, half)),
            dma((2, half)),
            dma((rep_size,)),
            dma((rep_size,)),
        ],
        compiler_params=pltpu.CompilerParams(
            collective_id=0, has_side_effects=True, vmem_limit_bytes=LIMIT
        ),
    )(
        values,
        out_weight.reshape(slices, cols // slices, outs),
        owners.reshape(1, tiles),
        subgroup.reshape(1, tiles),
        col_gain[None, :],
        col_bias[None, :],
    )
    return pl.pallas_call(
        finish,
        out_shape=jax.ShapeDtypeStruct((block_rows, outs), bf16),
        in_specs=[vmem, vmem, vmem],
        out_specs=hbm,
        scratch_shapes=[pltpu.VMEM((chunk, outs), bf16), dma((CHUNKS,))],
        compiler_params=pltpu.CompilerParams(vmem_limit_bytes=LIMIT_LAST),
    )(early, last_scored, weights)


def solution(mesh):
    return jax.shard_map(
        functools.partial(on_device, mesh.shape["shuf"], mesh.shape["rep"]),
        mesh=mesh,
        in_specs=(P("shuf", "rep"), P("shuf"), P("shuf", None), P("rep"), P("rep"), P("rep", None)),
        out_specs=P(("shuf", "rep"), None),
        check_vma=False,
    )
```
